256 devices in a mesh: group: 2 (over y_hi), fsdp: 128 (over x, z, y_lo, core).
Axes of the slice: x: 4, y: 4 (y_hi: 2, y_lo: 2; y = y_hi * 2 + y_lo), z: 8, core: 2. Of those that a mesh axis runs over, the one named last changes fastest.
Arguments:
- acts: bfloat16 [2, 65536, 8192], P('group', 'fsdp'), may hold values from -24 to 24
- cotangent: bfloat16 [2, 65536, 512], P('group', 'fsdp'), may hold values from -15.3125 to 15.3125
- inner_params: float32 [2, 8192, 512], P('group', 'fsdp'), may hold values from -6 to 6
- adam_first: float32 [2, 8192, 512], P('group', 'fsdp'), may hold values from -0.018 to 0.018
- adam_second: float32 [2, 8192, 512], P('group', 'fsdp'), may hold values from 1e-06 to 0.0001
- inner_steps: int32 [2], replicated, may hold values from 8 to 128
- group_tokens: int32 [2], replicated, may hold values from 16384 to 131072
- anchor: float32 [8192, 512], P(('fsdp', 'group')), may hold values from -6 to 6
- momentum: float32 [8192, 512], P(('fsdp', 'group')), may hold values from -2 to 2
Outputs:
- new_anchor: float32 [8192, 512], P(('fsdp', 'group'))
- new_momentum: float32 [8192, 512], P(('fsdp', 'group'))
- group_weights: bfloat16 [2, 8192, 512], P('group', 'fsdp')
The draws below stay inside these ranges and needn't reach their ends.
All inputs are finite; a program needn't handle non-finite values.
Results may differ from the reference program's by a relative error of at most 0.0004.
Values may be sent and summed in bfloat16 or wider, within the bound.
No kernel may reach another device: no remote copies, remote signals or barrier semaphores. Data moves between devices by JAX's collectives and lax.ppermute only.
A program may use at most 128 MiB of HBM per device.

```python
import math
import jax
import jax.numpy as jnp

D = 8192
KV = 512
TOK_DEV = 512
TOKG = 65536
N_GROUP = 2
N_FSDP = 128


def strengthened(values, rng, source, target, blocks, factor):
    def block_of(position):
        return (jnp.arange(values.shape[position]) // (values.shape[position] // blocks)).reshape((-1,) + (1,) * (values.ndim - 1 - position))

    first = jax.random.permutation(rng, blocks)[block_of(target)]
    far = (block_of(target) + blocks // 2) % blocks
    return jnp.where((block_of(source) == first) | (block_of(source) == far), factor * values, values)


def shard_levels(key, shape, pieces, low, high):
    def one(position, shards_of):
        heights = jax.random.uniform(jax.random.fold_in(jax.random.fold_in(key, 6), position), (shards_of,), jnp.float32, low / len(pieces), high / len(pieces))
        return jnp.repeat(jnp.exp(heights), shape[position] // shards_of).reshape((-1,) + (1,) * (len(shape) - position - 1))

    gain = one(*pieces[0])
    for cut in pieces[1:]:
        gain = gain * one(*cut)
    return gain


def normal_values(key, shape, deviation, bound, shards=(), held_as=jnp.bfloat16):
    values = jax.random.normal(key, shape, jnp.float32) * deviation
    if len(shards) > 0:
        values = shard_levels(key, shape, shards, -0.22, 0.18) * values
    return jnp.clip(values, min=-bound, max=bound).astype(held_as)


def gaussian_with(own_key, extent, deviation, bound, shards, heavy, kind=jnp.bfloat16):
    array = deviation * jax.random.normal(own_key, extent, jnp.float32)
    if shards:
        array = array * shard_levels(own_key, extent, shards, -0.22, 0.18)
    return jnp.clip(strengthened(array, jax.random.fold_in(own_key, 3), *heavy), -bound, bound).astype(kind)


def setup_inputs(seed: int = 0) -> dict:
    seeds = jax.random.split(jax.random.key(seed), 10)
    return {
        "acts": gaussian_with(seeds[0], (N_GROUP, TOKG, D), 1.0, 24.0, ((0, 2), (1, 128)), (1, 2, 128, 5.5)),
        "cotangent": normal_values(seeds[1], (N_GROUP, TOKG, KV), (0.01 * TOKG ** 0.5), 15.3125, ((0, 2), (1, 128))),
        "inner_params": normal_values(seeds[2], (N_GROUP, D, KV), 1.0, 6.0, ((0, 2), (1, 128)), jnp.float32),
        "adam_first": normal_values(seeds[3], (N_GROUP, D, KV), 0.003, 0.018, ((0, 2), (1, 128)), jnp.float32),
        "adam_second": jnp.clip(jnp.exp(math.log(0.0001) - 4.6051702 * jax.random.uniform(seeds[4], (N_GROUP, D, KV), jnp.float32) ** shard_levels(seeds[4], (N_GROUP, D, KV), ((0, 2), (1, 128)), -0.2, 0.2)), 9.999999974752427e-07, 0.0001),
        "inner_steps": jax.random.randint(seeds[5], (N_GROUP,), 8, 129).astype(jnp.int32),
        "group_tokens": jax.random.randint(seeds[6], (N_GROUP,), 16384, 131073).astype(jnp.int32),
        "anchor": normal_values(seeds[7], (D, KV), 1.0, 6.0, ((0, 256),), jnp.float32),
        "momentum": normal_values(seeds[8], (D, KV), 0.3, 2.0, ((0, 256),), jnp.float32),
    }


beta_one = 0.9
beta_two = 0.95
epsilon = 1e-08
inner_rate = 0.3
decay_rate = 0.1
outer_rate = 0.7
outer_mom = 0.9

def inner_update(params, first_moment, second_moment, gradient, steps):
    fresh_first = beta_one * first_moment + (1.0 - beta_one) * gradient
    fresh_second = beta_two * second_moment + (1.0 - beta_two) * gradient * gradient
    steps_float = steps.astype(jnp.float32)
    correct_one = 1.0 - jnp.power(jnp.float32(beta_one), steps_float)
    correct_two = 1.0 - jnp.power(jnp.float32(beta_two), steps_float)
    ratio = fresh_first / correct_one / (jnp.sqrt(fresh_second / correct_two) + epsilon)
    return params - inner_rate * (ratio + decay_rate * params)

def outer_update(anchor, momentum, merged):
    pseudo = anchor - merged
    fresh_momentum = outer_mom * momentum + pseudo
    fresh_anchor = anchor - outer_rate * (pseudo + outer_mom * fresh_momentum)
    return (fresh_anchor, fresh_momentum)

def reference(acts, cotangent, inner_params, adam_first, adam_second, inner_steps, group_tokens, anchor, momentum):
    counts = group_tokens.astype(jnp.float32)
    shares = counts / jnp.sum(counts)
    merged = jnp.zeros((D, KV), jnp.float32)
    for member in range(N_GROUP):
        gradient = jnp.dot(acts[member].T, cotangent[member], preferred_element_type=jnp.float32) / (TOK_DEV * N_FSDP)
        updated = inner_update(inner_params[member], adam_first[member], adam_second[member], gradient, inner_steps[member])
        merged = merged + shares[member] * updated
    new_anchor, new_momentum = outer_update(anchor, momentum, merged)
    group_weights = jnp.broadcast_to(new_anchor.astype(jnp.bfloat16)[None], (N_GROUP, D, KV))
    return (new_anchor, new_momentum, group_weights)
```

```python
import functools

import jax
import jax.numpy as jnp
from jax import lax
from jax.experimental import pallas as pl
from jax.experimental.pallas import tpu as pltpu
from jax.sharding import Mesh
from jax.sharding import PartitionSpec as P

FSDP = ("x", "z", "y", "c")
FSDP_GROUP = ("x", "z", "y", "c", "group")
NX, NZ, NY, NC, NG = 4, 8, 2, 2, 2

beta_one = 0.9
beta_two = 0.95
epsilon = 1e-08
inner_rate = 0.3
decay_rate = 0.1
outer_rate = 0.7
outer_mom = 0.9

WIRE = jnp.float16
F32 = jnp.float32
PEAK = 128.0
ROWS_A = 176
LANES = 128
BLOCK = 1024


def swap(a, axis):
    return lax.ppermute(a, axis, [(0, 1), (1, 0)])


def around(a, axis, k, size):
    return lax.ppermute(a, axis, [(i, (i + k) % size) for i in range(size)])


def pick(a, i):
    return lax.dynamic_index_in_dim(a, i, 0, False)


def terms_kernel(scale, which, cot, acts, out_a, out_b, turned):
    @pl.when(pl.program_id(0) == 0)
    def _():
        turned[...] = cot[...].astype(F32).T.astype(cot.dtype)

    out = jnp.dot(turned[...], acts[...], preferred_element_type=F32) * scale
    for j in range(BLOCK // LANES):
        z, y = divmod(j, NY)
        piece = out[:, j * LANES : (j + 1) * LANES]
        out_a[0, z, y] = piece[:ROWS_A]
        out_b[z, 0, y] = piece[ROWS_A:]


def terms(inputs, upstream, which):
    tokens, width = inputs.shape
    half = upstream.shape[1] // NC
    zs = BLOCK // (LANES * NY)
    per = NZ // zs
    rows_b = half - ROWS_A
    return pl.pallas_call(
        functools.partial(terms_kernel, PEAK / (tokens * NC)),
        grid_spec=pltpu.PrefetchScalarGridSpec(
            num_scalar_prefetch=1,
            grid=(width // BLOCK,),
            in_specs=[
                pl.BlockSpec((tokens, half), lambda i, w: (0, w[0])),
                pl.BlockSpec((tokens, BLOCK), lambda i, w: (0, i)),
            ],
            out_specs=[
                pl.BlockSpec(
                    (1, zs, NY, ROWS_A, LANES),
                    lambda i, w: (i // per, i % per, 0, 0, 0),
                ),
                pl.BlockSpec(
                    (zs, 1, NY, rows_b, LANES),
                    lambda i, w: (i % per, i // per, 0, 0, 0),
                ),
            ],
            scratch_shapes=[pltpu.VMEM((half, tokens), inputs.dtype)],
        ),
        out_shape=[
            jax.ShapeDtypeStruct((NX, NZ, NY, ROWS_A, LANES), F32),
            jax.ShapeDtypeStruct((NZ, NX, NY, rows_b, LANES), F32),
        ],
        cost_estimate=pl.CostEstimate(
            flops=2 * tokens * half * width,
            bytes_accessed=2 * tokens * width + 4 * half * width,
            transcendentals=0,
        ),
        name="terms",
    )(which[None], upstream, inputs)


def turn_kernel(first, second, out):
    rows = LANES // NC
    for y in range(NY):
        whole = jnp.concatenate([first[y], second[y]], 0).T
        for c in range(NC):
            for g in range(NG):
                out[(g * NY + y) * NC + c] = whole[c * rows : (c + 1) * rows]


def final_kernel(
    group, facts, got, p0, m0, v0, p1, m1, v1, a0, a1, w0, w1, new_a, new_m, new_w
):
    mine = group[0] == 0

    def weighted(first, k, p, m, v):
        at = [(g * NY + y) * NC for g in range(NG) for y in range(NY)]
        sides = []
        for c in range(NC):
            zero = got[at[0] + c] + got[at[1] + c]
            one = got[at[2] + c] + got[at[3] + c]
            sides.append(jnp.where(mine == first, zero, one))
        gradient = jnp.concatenate(sides, -1) * (1.0 / (NY * PEAK))
        share, correct_one, correct_two = (facts[3 * k + n] for n in range(3))
        fresh_first = beta_one * m + (1.0 - beta_one) * gradient
        fresh_second = beta_two * v + (1.0 - beta_two) * gradient * gradient
        ratio = (
            fresh_first / correct_one / (jnp.sqrt(fresh_second / correct_two) + epsilon)
        )
        return share * (p - inner_rate * (ratio + decay_rate * p))

    merged = weighted(True, 0, p0[...], m0[...], v0[...]) + weighted(
        False, 1, p1[...], m1[...], v1[...]
    )
    few = a0.shape[0]

    def half(anchor, momentum, part):
        pseudo = anchor - part
        fresh_momentum = outer_mom * momentum + pseudo
        fresh_anchor = anchor - outer_rate * (pseudo + outer_mom * fresh_momentum)
        return fresh_anchor, fresh_momentum

    front, back = merged[:few], merged[few:]
    near_anchor, near_momentum = half(a0[...], w0[...], jnp.where(mine, front, back))
    far_anchor, _ = half(a1[...], w1[...], jnp.where(mine, back, front))
    new_a[...] = near_anchor
    new_m[...] = near_momentum
    new_w[:few] = jnp.where(mine, near_anchor, far_anchor).astype(new_w.dtype)
    new_w[few:] = jnp.where(mine, far_anchor, near_anchor).astype(new_w.dtype)


def per_device(
    acts,
    cotangent,
    inner_params,
    adam_first,
    adam_second,
    inner_steps,
    group_tokens,
    anchor,
    momentum,
):
    group, x, z, core = (lax.axis_index(a) for a in ("group", "x", "z", "c"))
    inputs = acts[0]
    upstream = cotangent[0]
    half = upstream.shape[1] // NC
    rows = inner_params.shape[1]

    theirs_a, theirs_b = terms(inputs, upstream, 1 - core)
    with jax.named_scope("core"):
        got_a = swap(theirs_a, "c")
        got_b = swap(theirs_b, "c")
    near = (inner_params[0], adam_first[0], adam_second[0], anchor, momentum)
    gated, inputs, upstream, _ = lax.optimization_barrier(
        (near, inputs, upstream, theirs_a)
    )
    with jax.named_scope("state"):
        far = tuple(swap(a, "group") for a in gated)
    own_a, own_b = terms(inputs, upstream, core)

    def chip_a(i):
        return pick(own_a, i) + pick(got_a, i)

    with jax.named_scope("xa"):
        sent = [
            around(chip_a((x + k) % NX).astype(WIRE), "x", k, NX) for k in (2, 1, 3)
        ]
    second = own_b + got_b
    with jax.named_scope("zb"):
        back = lax.all_to_all(second.astype(WIRE), "z", 0, 0, tiled=True)
    first = chip_a(x)
    sent, back = lax.optimization_barrier((sent, back))
    place = lax.broadcasted_iota(jnp.int32, (NZ, 1, 1, 1, 1), 0)
    back = jnp.where(place == z, 0.0, back.astype(F32)).sum(0) + pick(second, z)
    second = back * (1.0 / NZ)
    with jax.named_scope("xb"):
        sent_b = [
            around(pick(second, (x + k) % NX).astype(WIRE), "x", k, NX)
            for k in (2, 1, 3)
        ]
    second = pick(second, x)

    for s in sent:
        first = first + s.astype(F32)
    first = first * (1.0 / NX)
    with jax.named_scope("za"):
        back = lax.all_to_all(first.astype(WIRE), "z", 0, 0, tiled=True)
    sent_b, back = lax.optimization_barrier((sent_b, back))
    place = lax.broadcasted_iota(jnp.int32, (NZ, 1, 1, 1), 0)
    first = jnp.where(place == z, 0.0, back.astype(F32)).sum(0) + pick(first, z)
    first = first * (1.0 / NZ)
    for s in sent_b:
        second = second + s.astype(F32)
    second = second * (1.0 / NX)

    part = pl.pallas_call(
        turn_kernel,
        out_shape=jax.ShapeDtypeStruct((NG * NY * NC, rows, half), F32),
        name="turn",
    )(first, second)
    with jax.named_scope("last"):
        got = lax.all_to_all(part, ("group", "y", "c"), 0, 0, tiled=True)

    counts = group_tokens.astype(F32)
    steps = inner_steps.astype(F32)
    facts = jnp.stack(
        [
            counts / jnp.sum(counts),
            1.0 - jnp.power(F32(beta_one), steps),
            1.0 - jnp.power(F32(beta_two), steps),
        ],
        1,
    )
    facts = jnp.where(group == 0, facts, facts[::-1]).reshape(-1)
    vmem = pl.BlockSpec(memory_space=pltpu.VMEM)
    smem = pl.BlockSpec(memory_space=pltpu.SMEM)
    new_anchor, new_momentum, weights = pl.pallas_call(
        final_kernel,
        in_specs=[smem, smem] + [vmem] * 11,
        out_specs=[vmem] * 3,
        out_shape=[
            jax.ShapeDtypeStruct(anchor.shape, F32),
            jax.ShapeDtypeStruct(anchor.shape, F32),
            jax.ShapeDtypeStruct((rows, anchor.shape[1]), jnp.bfloat16),
        ],
        name="final",
    )(
        group[None],
        facts,
        got,
        *near[:3],
        *far[:3],
        near[3],
        far[3],
        near[4],
        far[4],
    )
    return new_anchor, new_momentum, weights[None]


def solution(mesh):
    torus = Mesh(
        mesh.devices.reshape(NG, NX, NZ, NY, NC), ("group", "x", "z", "y", "c")
    )
    shard = P("group", FSDP, None)
    thin = P(FSDP_GROUP, None)
    return jax.shard_map(
        per_device,
        mesh=torus,
        in_specs=(shard, shard, shard, shard, shard, P(), P(), thin, thin),
        out_specs=(thin, thin, shard),
        check_vma=False,
    )
```

```python
import functools

import jax
import jax.numpy as jnp
from jax import lax
from jax.experimental import pallas as pl
from jax.experimental.pallas import tpu as pltpu
from jax.sharding import Mesh
from jax.sharding import PartitionSpec as P

FSDP = ("x", "z", "y", "c")
FSDP_GROUP = ("x", "z", "y", "c", "group")
NX, NZ, NY, NC, NG = 4, 8, 2, 2, 2

beta_one = 0.9
beta_two = 0.95
epsilon = 1e-08
inner_rate = 0.3
decay_rate = 0.1
outer_rate = 0.7
outer_mom = 0.9

WIRE = jnp.float16
F32 = jnp.float32
PEAK = 128.0
ROWS_A = 192
LANES = 128
BLOCK = 1024
ORDER = (2, 1, 3, 0)


def swap(a, axis):
    return lax.ppermute(a, axis, [(0, 1), (1, 0)])


def around(a, axis, k, size):
    return lax.ppermute(a, axis, [(i, (i + k) % size) for i in range(size)])


def pick(a, i):
    return lax.dynamic_index_in_dim(a, i, 0, False)


def terms_kernel(scale, which, place, cot, acts, *refs):
    outs, out_b = refs[:NX], refs[NX]
    turned, held, arrived = refs[NX + 1 :]
    step = pl.program_id(0)
    steps = acts.shape[1] // BLOCK
    per = steps // NX

    def copy(i):
        x = lax.rem(place[0] + ORDER[i // per], NX)
        start = pl.multiple_of((x * per + i % per) * BLOCK, BLOCK)
        return pltpu.make_async_copy(
            acts.at[:, pl.ds(start, BLOCK)], held.at[i], arrived.at[i]
        )

    @pl.when(step == 0)
    def _():
        for i in range(steps):
            copy(i).start()
        turned[...] = cot[...].astype(F32).T.astype(cot.dtype)

    for i in range(steps):

        @pl.when(step == i)
        def _():
            copy(i).wait()
            out = jnp.dot(turned[...], held[i], preferred_element_type=F32) * scale
            for j in range(BLOCK // LANES):
                z, y = divmod(j, NY)
                piece = out[:, j * LANES : (j + 1) * LANES]
                outs[i // per][z, y] = piece[:ROWS_A]
                out_b[z, 0, y] = piece[ROWS_A:]


def terms(inputs, upstream, which, x):
    tokens, width = inputs.shape
    half = upstream.shape[1] // NC
    zs = BLOCK // (LANES * NY)
    per = NZ // zs
    steps = width // BLOCK
    rows_b = half - ROWS_A

    def at(n):
        return lambda i, w, x: (jnp.clip(i - n * per, 0, per - 1), 0, 0, 0)

    return pl.pallas_call(
        functools.partial(terms_kernel, PEAK / (tokens * NC)),
        grid_spec=pltpu.PrefetchScalarGridSpec(
            num_scalar_prefetch=2,
            grid=(steps,),
            in_specs=[
                pl.BlockSpec((tokens, half), lambda i, w, x: (0, w[0])),
                pl.BlockSpec(memory_space=pl.ANY),
            ],
            out_specs=[
                pl.BlockSpec((zs, NY, ROWS_A, LANES), at(n)) for n in range(NX)
            ]
            + [
                pl.BlockSpec(
                    (zs, 1, NY, rows_b, LANES),
                    lambda i, w, x: (i % per, i // per, 0, 0, 0),
                ),
            ],
            scratch_shapes=[
                pltpu.VMEM((half, tokens), inputs.dtype),
                pltpu.VMEM((steps, tokens, BLOCK), inputs.dtype),
                pltpu.SemaphoreType.DMA((steps,)),
            ],
        ),
        out_shape=[jax.ShapeDtypeStruct((NZ, NY, ROWS_A, LANES), F32)] * NX
        + [jax.ShapeDtypeStruct((NZ, NX, NY, rows_b, LANES), F32)],
        cost_estimate=pl.CostEstimate(
            flops=2 * tokens * half * width,
            bytes_accessed=2 * tokens * width + 4 * half * width,
            transcendentals=0,
        ),
        name="terms",
    )(which[None], x[None], upstream, inputs)


def turn_kernel(first, second, out):
    rows = LANES // NC
    for y in range(NY):
        whole = jnp.concatenate([first[y], second[y]], 0).T
        for c in range(NC):
            for g in range(NG):
                out[(g * NY + y) * NC + c] = whole[c * rows : (c + 1) * rows]


def pack_kernel(*refs):
    at = 0
    for ref in refs[:-1]:
        refs[-1][at : at + ref.shape[0]] = ref[...]
        at += ref.shape[0]


def final_kernel(group, facts, got, p0, m0, v0, a0, w0, far, new_a, new_m, new_w):
    rows, few = p0.shape[0], a0.shape[0]
    p1, m1, v1 = (far[i * rows : (i + 1) * rows] for i in range(3))
    a1, w1 = far[3 * rows : 3 * rows + few], far[3 * rows + few :]
    mine = group[0] == 0

    def weighted(first, k, p, m, v):
        at = [(g * NY + y) * NC for g in range(NG) for y in range(NY)]
        sides = []
        for c in range(NC):
            zero = got[at[0] + c] + got[at[1] + c]
            one = got[at[2] + c] + got[at[3] + c]
            sides.append(jnp.where(mine == first, zero, one))
        gradient = jnp.concatenate(sides, -1) * (1.0 / (NY * PEAK))
        share, correct_one, correct_two = (facts[3 * k + n] for n in range(3))
        fresh_first = beta_one * m + (1.0 - beta_one) * gradient
        fresh_second = beta_two * v + (1.0 - beta_two) * gradient * gradient
        ratio = (
            fresh_first / correct_one / (jnp.sqrt(fresh_second / correct_two) + epsilon)
        )
        return share * (p - inner_rate * (ratio + decay_rate * p))

    merged = weighted(True, 0, p0[...], m0[...], v0[...]) + weighted(
        False, 1, p1, m1, v1
    )

    def half(anchor, momentum, part):
        pseudo = anchor - part
        fresh_momentum = outer_mom * momentum + pseudo
        fresh_anchor = anchor - outer_rate * (pseudo + outer_mom * fresh_momentum)
        return fresh_anchor, fresh_momentum

    front, back = merged[:few], merged[few:]
    near_anchor, near_momentum = half(a0[...], w0[...], jnp.where(mine, front, back))
    far_anchor, _ = half(a1, w1, jnp.where(mine, back, front))
    new_a[...] = near_anchor
    new_m[...] = near_momentum
    new_w[:few] = jnp.where(mine, near_anchor, far_anchor).astype(new_w.dtype)
    new_w[few:] = jnp.where(mine, far_anchor, near_anchor).astype(new_w.dtype)


def per_device(
    acts,
    cotangent,
    inner_params,
    adam_first,
    adam_second,
    inner_steps,
    group_tokens,
    anchor,
    momentum,
):
    group, x, z, core = (lax.axis_index(a) for a in ("group", "x", "z", "c"))
    inputs = acts[0]
    upstream = cotangent[0]
    half = upstream.shape[1] // NC
    rows = inner_params.shape[1]

    *theirs_a, theirs_b = terms(inputs, upstream, 1 - core, x)
    got_a = [swap(a, "c") for a in theirs_a]
    got_b = swap(theirs_b, "c")
    inputs, upstream, _ = lax.optimization_barrier((inputs, upstream, theirs_b))
    *own_a, own_b = terms(inputs, upstream, core, x)
    counts = group_tokens.astype(F32)
    steps = inner_steps.astype(F32)
    facts = jnp.stack(
        [
            counts / jnp.sum(counts),
            1.0 - jnp.power(F32(beta_one), steps),
            1.0 - jnp.power(F32(beta_two), steps),
        ],
        1,
    )
    facts = jnp.where(group == 0, facts, facts[::-1]).reshape(-1)

    def wire_a(n):
        return (own_a[n] + got_a[n]).astype(WIRE)

    near = (inner_params[0], adam_first[0], adam_second[0], anchor, momentum)

    def send_a(n):
        return around(wire, "x", ORDER[n], NX)

    wire = wire_a(0)
    sent = [send_a(0)]
    _, own_b, got_b = lax.optimization_barrier((wire, own_b, got_b))
    wire = wire_b = (own_b + got_b).astype(WIRE)
    back = lax.all_to_all(wire_b, "z", 0, 0, tiled=True)
    for n in range(1, NX - 1):
        _, own_a[n], got_a[n] = lax.optimization_barrier((wire, own_a[n], got_a[n]))
        wire = wire_a(n)
        sent.append(send_a(n))
    gated, _ = lax.optimization_barrier((near, wire))
    packed = pl.pallas_call(
        pack_kernel,
        out_shape=jax.ShapeDtypeStruct(
            (sum(a.shape[0] for a in near), near[0].shape[1]), F32
        ),
        name="pack",
    )(*gated)
    far = swap(packed, "group")
    first = own_a[-1] + got_a[-1]
    second = pick(own_b, z) + pick(got_b, z)
    sent, back, far, facts = lax.optimization_barrier((sent, back, far, facts))
    place = lax.broadcasted_iota(jnp.int32, (NZ, 1, 1, 1, 1), 0)
    second = jnp.where(place == z, 0.0, back.astype(F32)).sum(0) + second
    second = second * (1.0 / NZ)
    sent_b = [around(second[n].astype(WIRE), "x", ORDER[n], NX) for n in range(NX - 1)]
    second = second[-1]

    for s in sent:
        first = first + s.astype(F32)
    first = first * (1.0 / NX)
    back = lax.all_to_all(first.astype(WIRE), "z", 0, 0, tiled=True)
    sent_b, back = lax.optimization_barrier((sent_b, back))
    place = lax.broadcasted_iota(jnp.int32, (NZ, 1, 1, 1), 0)
    first = jnp.where(place == z, 0.0, back.astype(F32)).sum(0) + pick(first, z)
    first = first * (1.0 / NZ)
    for s in sent_b:
        second = second + s.astype(F32)
    second = second * (1.0 / NX)

    part = pl.pallas_call(
        turn_kernel,
        out_shape=jax.ShapeDtypeStruct((NG * NY * NC, rows, half), F32),
        name="turn",
    )(first, second)
    got = lax.all_to_all(part, ("group", "y", "c"), 0, 0, tiled=True)

    vmem = pl.BlockSpec(memory_space=pltpu.VMEM)
    smem = pl.BlockSpec(memory_space=pltpu.SMEM)
    new_anchor, new_momentum, weights = pl.pallas_call(
        final_kernel,
        in_specs=[smem, smem] + [vmem] * 7,
        out_specs=[vmem] * 3,
        out_shape=[
            jax.ShapeDtypeStruct(anchor.shape, F32),
            jax.ShapeDtypeStruct(anchor.shape, F32),
            jax.ShapeDtypeStruct((rows, anchor.shape[1]), jnp.bfloat16),
        ],
        name="final",
    )(group[None], facts, got, *near, far)
    return new_anchor, new_momentum, weights[None]


def solution(mesh):
    torus = Mesh(
        mesh.devices.reshape(NG, NX, NZ, NY, NC), ("group", "x", "z", "y", "c")
    )
    shard = P("group", FSDP, None)
    thin = P(FSDP_GROUP, None)

    return jax.shard_map(
        per_device,
        mesh=torus,
        in_specs=(shard, shard, shard, shard, shard, P(), P(), thin, thin),
        out_specs=(thin, thin, shard),
        check_vma=False,
    )
```

```python
import functools

import jax
import jax.numpy as jnp
from jax import lax
from jax.experimental import pallas as pl
from jax.experimental.pallas import tpu as pltpu
from jax.sharding import Mesh
from jax.sharding import PartitionSpec as P

FSDP = ("x", "z", "y", "c")
FSDP_GROUP = ("x", "z", "y", "c", "group")
NX, NZ, NY, NC, NG = 4, 8, 2, 2, 2

beta_one = 0.9
beta_two = 0.95
epsilon = 1e-08
inner_rate = 0.3
decay_rate = 0.1
outer_rate = 0.7
outer_mom = 0.9

WIRE = jnp.float16
F32 = jnp.float32
PEAK = 128.0
ROWS_A = 184
LANES = 128
BLOCK = 1024
AHEAD = 4
ORDER = (2, 1, 3, 0)


def swap(a, axis):
    return lax.ppermute(a, axis, [(0, 1), (1, 0)])


def around(a, axis, k, size):
    return lax.ppermute(a, axis, [(i, (i + k) % size) for i in range(size)])


def pick(a, i):
    return lax.dynamic_index_in_dim(a, i, 0, False)


def terms_kernel(scale, which, place, cot, acts, *refs):
    outs, out_b = refs[:NX], refs[NX]
    upstream, held, mine, arrived, ready, left = refs[NX + 1 :]
    outs = (*outs[:-1], mine)
    last = pltpu.make_async_copy(mine, refs[NX - 1], left)
    steps = acts.shape[1] // BLOCK
    per = steps // NX
    half = upstream.shape[1]

    turns = [n * per + i for n in (0, NX - 1, *range(1, NX - 1)) for i in range(per)]

    def copy(i):
        x = lax.rem(place[0] + ORDER[i // per], NX)
        start = pl.multiple_of((x * per + i % per) * BLOCK, BLOCK)
        return pltpu.make_async_copy(
            acts.at[:, pl.ds(start, BLOCK)], held.at[i], arrived.at[i]
        )

    first = pl.multiple_of(which[0] * half, half)
    whole = pltpu.make_async_copy(cot.at[:, pl.ds(first, half)], upstream, ready)
    whole.start()
    for i in turns[:AHEAD]:
        copy(i).start()
    whole.wait()
    turned = upstream[...].astype(F32).T.astype(upstream.dtype)
    for turn, i in enumerate(turns):
        copy(i).wait()
        if turn + AHEAD < steps:
            copy(turns[turn + AHEAD]).start()
        out = jnp.dot(turned, held[i], preferred_element_type=F32) * scale
        for j in range(BLOCK // LANES):
            z, y = divmod(j, NY)
            z += i % per * (NZ // per)
            piece = out[:, j * LANES : (j + 1) * LANES]
            outs[i // per][z, y] = piece[:ROWS_A]
            out_b[z, i // per, y] = piece[ROWS_A:]
        if turn == 2 * per - 1:
            last.start()
    last.wait()


def terms(inputs, upstream, which, x):
    tokens, width = inputs.shape
    half = upstream.shape[1] // NC
    steps = width // BLOCK
    vmem = pl.BlockSpec(memory_space=pltpu.VMEM)
    return pl.pallas_call(
        functools.partial(terms_kernel, PEAK / (tokens * NC)),
        in_specs=[pl.BlockSpec(memory_space=pltpu.SMEM)] * 2
        + [pl.BlockSpec(memory_space=pl.ANY)] * 2,
        out_specs=[vmem] * (NX - 1) + [pl.BlockSpec(memory_space=pl.ANY), vmem],
        scratch_shapes=[
            pltpu.VMEM((tokens, half), inputs.dtype),
            pltpu.VMEM((steps, tokens, BLOCK), inputs.dtype),
            pltpu.VMEM((NZ, NY, ROWS_A, LANES), F32),
            pltpu.SemaphoreType.DMA((steps,)),
            pltpu.SemaphoreType.DMA,
            pltpu.SemaphoreType.DMA,
        ],
        out_shape=[pltpu.VMEM((NZ, NY, ROWS_A, LANES), F32)] * (NX - 1)
        + [pltpu.HBM((NZ, NY, ROWS_A, LANES), F32)]
        + [pltpu.VMEM((NZ, NX, NY, half - ROWS_A, LANES), F32)],
        compiler_params=pltpu.CompilerParams(vmem_limit_bytes=18 * 2**20),
        cost_estimate=pl.CostEstimate(
            flops=2 * tokens * half * width,
            bytes_accessed=2 * tokens * width + 4 * half * width,
            transcendentals=0,
        ),
        name="terms",
    )(
        which[None],
        x[None],
        pltpu.with_memory_space_constraint(upstream, pltpu.HBM),
        pltpu.with_memory_space_constraint(inputs, pltpu.HBM),
    )


def turn_kernel(first, second, out):
    rows = LANES // NC
    for y in range(NY):
        whole = jnp.concatenate([first[y], second[y]], 0).T
        for c in range(NC):
            for g in range(NG):
                out[(g * NY + y) * NC + c] = whole[c * rows : (c + 1) * rows]


def pack_kernel(*refs):
    at = 0
    for ref in refs[:-1]:
        refs[-1][at : at + ref.shape[0]] = ref[...]
        at += ref.shape[0]


def final_kernel(group, facts, got, p0, m0, v0, a0, w0, far, new_a, new_m, new_w):
    rows, few = p0.shape[0], a0.shape[0]
    p1, m1, v1 = (far[i * rows : (i + 1) * rows] for i in range(3))
    a1, w1 = far[3 * rows : 3 * rows + few], far[3 * rows + few :]
    mine = group[0] == 0

    def weighted(first, k, p, m, v):
        at = [(g * NY + y) * NC for g in range(NG) for y in range(NY)]
        sides = []
        for c in range(NC):
            zero = got[at[0] + c] + got[at[1] + c]
            one = got[at[2] + c] + got[at[3] + c]
            sides.append(jnp.where(mine == first, zero, one))
        gradient = jnp.concatenate(sides, -1) * (1.0 / (NY * PEAK))
        share, correct_one, correct_two = (facts[3 * k + n] for n in range(3))
        fresh_first = beta_one * m + (1.0 - beta_one) * gradient
        fresh_second = beta_two * v + (1.0 - beta_two) * gradient * gradient
        ratio = (
            fresh_first / correct_one / (jnp.sqrt(fresh_second / correct_two) + epsilon)
        )
        return share * (p - inner_rate * (ratio + decay_rate * p))

    merged = weighted(True, 0, p0[...], m0[...], v0[...]) + weighted(
        False, 1, p1, m1, v1
    )

    def half(anchor, momentum, part):
        pseudo = anchor - part
        fresh_momentum = outer_mom * momentum + pseudo
        fresh_anchor = anchor - outer_rate * (pseudo + outer_mom * fresh_momentum)
        return fresh_anchor, fresh_momentum

    front, back = merged[:few], merged[few:]
    near_anchor, near_momentum = half(a0[...], w0[...], jnp.where(mine, front, back))
    far_anchor, _ = half(a1, w1, jnp.where(mine, back, front))
    new_a[...] = near_anchor
    new_m[...] = near_momentum
    new_w[:few] = jnp.where(mine, near_anchor, far_anchor).astype(new_w.dtype)
    new_w[few:] = jnp.where(mine, far_anchor, near_anchor).astype(new_w.dtype)


def per_device(
    acts,
    cotangent,
    inner_params,
    adam_first,
    adam_second,
    inner_steps,
    group_tokens,
    anchor,
    momentum,
):
    group, x, z, core = (lax.axis_index(a) for a in ("group", "x", "z", "c"))
    inputs = acts[0]
    upstream = cotangent[0]
    half = upstream.shape[1] // NC
    rows = inner_params.shape[1]

    *theirs_a, theirs_b = terms(inputs, upstream, 1 - core, x)
    got_a = []
    for a in theirs_a:
        got_a.append(swap(a, "c"))
    got_b = swap(theirs_b, "c")
    inputs, upstream, _ = lax.optimization_barrier((inputs, upstream, theirs_b))
    *own_a, own_b = terms(inputs, upstream, core, x)
    counts = group_tokens.astype(F32)
    steps = inner_steps.astype(F32)
    facts = jnp.stack(
        [
            counts / jnp.sum(counts),
            1.0 - jnp.power(F32(beta_one), steps),
            1.0 - jnp.power(F32(beta_two), steps),
        ],
        1,
    )
    facts = jnp.where(group == 0, facts, facts[::-1]).reshape(-1)

    near = (inner_params[0], adam_first[0], adam_second[0], anchor, momentum)

    def send(wire, n):
        return around(wire, "x", ORDER[n], NX)

    wire = (own_a[0] + got_a[0]).astype(WIRE)
    sent_0 = send(wire, 0)
    _, own_b, got_b = lax.optimization_barrier((wire, own_b, got_b))
    wire = (own_b + got_b).astype(WIRE)
    back_b = lax.all_to_all(wire, "z", 0, 0, tiled=True)
    sent = [sent_0]
    for n in range(1, NX - 1):
        _, own, got = lax.optimization_barrier((wire, own_a[n], got_a[n]))
        wire = (own + got).astype(WIRE)
        sent.append(send(wire, n))
    gated, _ = lax.optimization_barrier((near, wire))
    packed = pl.pallas_call(
        pack_kernel,
        out_shape=jax.ShapeDtypeStruct(
            (sum(a.shape[0] for a in near), near[0].shape[1]), F32
        ),
        name="pack",
    )(*gated)
    far = swap(packed, "group")

    sent, back_b, far, facts = lax.optimization_barrier((sent, back_b, far, facts))
    first = own_a[-1] + got_a[-1]
    for w in sent:
        first = first + w.astype(F32)
    first = first * (1.0 / NX)
    back_a = lax.all_to_all(first.astype(WIRE), "z", 0, 0, tiled=True)
    second = back_b.astype(F32).sum(0) * (1.0 / NZ)
    wires = [second[n].astype(WIRE) for n in range(NX - 1)]
    sent_b = [around(wires[n], "x", ORDER[n], NX) for n in range(NX - 1)]
    second = second[-1]
    sent_b, back_a = lax.optimization_barrier((sent_b, back_a))
    for w in sent_b:
        second = second + w.astype(F32)
    second = second * (1.0 / NX)
    place = lax.broadcasted_iota(jnp.int32, (NZ, 1, 1, 1), 0)
    back_a = jnp.where(place == z, 0.0, back_a.astype(F32)).sum(0)
    first = (back_a + pick(first, z)) * (1.0 / NZ)

    part = pl.pallas_call(
        turn_kernel,
        out_shape=jax.ShapeDtypeStruct((NG * NY * NC, rows, half), F32),
        name="turn",
    )(first, second)
    got = lax.all_to_all(part, ("group", "y", "c"), 0, 0, tiled=True)

    vmem = pl.BlockSpec(memory_space=pltpu.VMEM)
    smem = pl.BlockSpec(memory_space=pltpu.SMEM)
    new_anchor, new_momentum, weights = pl.pallas_call(
        final_kernel,
        in_specs=[smem, smem] + [vmem] * 7,
        out_specs=[vmem] * 3,
        out_shape=[
            jax.ShapeDtypeStruct(anchor.shape, F32),
            jax.ShapeDtypeStruct(anchor.shape, F32),
            jax.ShapeDtypeStruct((rows, anchor.shape[1]), jnp.bfloat16),
        ],
        name="final",
    )(group[None], facts, got, *near, far)
    return new_anchor, new_momentum, weights[None]


def solution(mesh):
    torus = Mesh(
        mesh.devices.reshape(NG, NX, NZ, NY, NC), ("group", "x", "z", "y", "c")
    )
    shard = P("group", FSDP, None)
    thin = P(FSDP_GROUP, None)

    return jax.shard_map(
        per_device,
        mesh=torus,
        in_specs=(shard, shard, shard, shard, shard, P(), P(), thin, thin),
        out_specs=(thin, thin, shard),
        check_vma=False,
    )
```

```python
import functools

import jax
import jax.numpy as jnp
from jax import lax
from jax.experimental import pallas as pl
from jax.experimental.pallas import tpu as pltpu
from jax.sharding import Mesh
from jax.sharding import PartitionSpec as P


FSDP = ("x", "z", "y", "c")
FSDP_GROUP = ("x", "z", "y", "c", "group")
NX, NZ, NY, NC, NG = 4, 8, 2, 2, 2

beta_one = 0.9
beta_two = 0.95
epsilon = 1e-08
inner_rate = 0.3
decay_rate = 0.1
outer_rate = 0.7
outer_mom = 0.9

WIRE = jnp.float16
F32 = jnp.float32
PEAK = 128.0
ROWS_A = 176
LANES = 128
BLOCK = 1024
AHEAD = 4
ORDER = (2, 1, 3, 0)
FAR = (4, 3, 5, 2, 6, 1, 7)


def swap(a, axis):
    return lax.ppermute(a, axis, [(0, 1), (1, 0)])


def around(a, axis, k, size):
    return lax.ppermute(a, axis, [(i, (i + k) % size) for i in range(size)])


def terms_kernel(scale, which, place, layer, cot, acts, *refs):
    outs, out_b = refs[:NX], refs[NX]
    upstream, held, mine, arrived, ready, left = refs[NX + 1 :]
    outs = (*outs[:-1], mine)
    last = pltpu.make_async_copy(mine, refs[NX - 1], left)
    steps = acts.shape[1] // BLOCK
    per = steps // NX
    half = upstream.shape[1]

    turns = [n * per + i for n in (0, NX - 1, *range(1, NX - 1)) for i in range(per)]

    def copy(i):
        x = lax.rem(place[0] + ORDER[i // per], NX)
        start = pl.multiple_of((x * per + i % per) * BLOCK, BLOCK)
        return pltpu.make_async_copy(
            acts.at[:, pl.ds(start, BLOCK)], held.at[i], arrived.at[i]
        )

    first = pl.multiple_of(which[0] * half, half)
    whole = pltpu.make_async_copy(cot.at[:, pl.ds(first, half)], upstream, ready)
    whole.start()
    for i in turns[:AHEAD]:
        copy(i).start()
    whole.wait()
    turned = upstream[...].astype(F32).T.astype(upstream.dtype)
    for turn, i in enumerate(turns):
        copy(i).wait()
        if turn + AHEAD < steps:
            copy(turns[turn + AHEAD]).start()
        out = jnp.dot(turned, held[i], preferred_element_type=F32) * scale
        for j in range(BLOCK // LANES):
            z, y = divmod(j, NY)
            z += i % per * (NZ // per)
            z = lax.rem(z + NZ - layer[0], NZ)
            piece = out[:, j * LANES : (j + 1) * LANES]
            outs[i // per][z, y] = piece[:ROWS_A]
            out_b[z, i // per, y] = piece[ROWS_A:]
        if turn == 2 * per - 1:
            last.start()
    last.wait()


def terms(inputs, upstream, which, x, z):
    tokens, width = inputs.shape
    half = upstream.shape[1] // NC
    steps = width // BLOCK
    vmem = pl.BlockSpec(memory_space=pltpu.VMEM)
    return pl.pallas_call(
        functools.partial(terms_kernel, PEAK / (tokens * NC)),
        in_specs=[pl.BlockSpec(memory_space=pltpu.SMEM)] * 3
        + [pl.BlockSpec(memory_space=pl.ANY)] * 2,
        out_specs=[vmem] * (NX - 1) + [pl.BlockSpec(memory_space=pl.ANY), vmem],
        scratch_shapes=[
            pltpu.VMEM((tokens, half), inputs.dtype),
            pltpu.VMEM((steps, tokens, BLOCK), inputs.dtype),
            pltpu.VMEM((NZ, NY, ROWS_A, LANES), F32),
            pltpu.SemaphoreType.DMA((steps,)),
            pltpu.SemaphoreType.DMA,
            pltpu.SemaphoreType.DMA,
        ],
        out_shape=[pltpu.VMEM((NZ, NY, ROWS_A, LANES), F32)] * (NX - 1)
        + [pltpu.HBM((NZ, NY, ROWS_A, LANES), F32)]
        + [pltpu.VMEM((NZ, NX, NY, half - ROWS_A, LANES), F32)],
        compiler_params=pltpu.CompilerParams(vmem_limit_bytes=18 * 2**20),
        cost_estimate=pl.CostEstimate(
            flops=2 * tokens * half * width,
            bytes_accessed=2 * tokens * width + 4 * half * width,
            transcendentals=0,
        ),
        name="terms",
    )(
        which[None],
        x[None],
        z[None],
        pltpu.with_memory_space_constraint(upstream, pltpu.HBM),
        pltpu.with_memory_space_constraint(inputs, pltpu.HBM),
    )


def turn_kernel(first, second, out):
    rows = LANES // NC
    for y in range(NY):
        whole = jnp.concatenate([first[y], second[y]], 0).T
        for c in range(NC):
            for g in range(NG):
                out[(g * NY + y) * NC + c] = whole[c * rows : (c + 1) * rows]


def pack_kernel(*refs):
    at = 0
    for ref in refs[:-1]:
        refs[-1][at : at + ref.shape[0]] = ref[...]
        at += ref.shape[0]


def final_kernel(group, facts, got, p0, m0, v0, a0, w0, far, new_a, new_m, new_w):
    rows, few = p0.shape[0], a0.shape[0]
    p1, m1, v1 = (far[i * rows : (i + 1) * rows] for i in range(3))
    a1, w1 = far[3 * rows : 3 * rows + few], far[3 * rows + few :]
    mine = group[0] == 0

    def weighted(first, k, p, m, v):
        at = [(g * NY + y) * NC for g in range(NG) for y in range(NY)]
        sides = []
        for c in range(NC):
            zero = got[at[0] + c] + got[at[1] + c]
            one = got[at[2] + c] + got[at[3] + c]
            sides.append(jnp.where(mine == first, zero, one))
        gradient = jnp.concatenate(sides, -1) * (1.0 / (NY * PEAK))
        share, correct_one, correct_two = (facts[3 * k + n] for n in range(3))
        fresh_first = beta_one * m + (1.0 - beta_one) * gradient
        fresh_second = beta_two * v + (1.0 - beta_two) * gradient * gradient
        ratio = (
            fresh_first / correct_one / (jnp.sqrt(fresh_second / correct_two) + epsilon)
        )
        return share * (p - inner_rate * (ratio + decay_rate * p))

    merged = weighted(True, 0, p0[...], m0[...], v0[...]) + weighted(
        False, 1, p1, m1, v1
    )

    def half(anchor, momentum, part):
        pseudo = anchor - part
        fresh_momentum = outer_mom * momentum + pseudo
        fresh_anchor = anchor - outer_rate * (pseudo + outer_mom * fresh_momentum)
        return fresh_anchor, fresh_momentum

    front, back = merged[:few], merged[few:]
    near_anchor, near_momentum = half(a0[...], w0[...], jnp.where(mine, front, back))
    far_anchor, _ = half(a1, w1, jnp.where(mine, back, front))
    new_a[...] = near_anchor
    new_m[...] = near_momentum
    new_w[:few] = jnp.where(mine, near_anchor, far_anchor).astype(new_w.dtype)
    new_w[few:] = jnp.where(mine, far_anchor, near_anchor).astype(new_w.dtype)


def per_device(
    acts,
    cotangent,
    inner_params,
    adam_first,
    adam_second,
    inner_steps,
    group_tokens,
    anchor,
    momentum,
):
    group, x, z, core = (lax.axis_index(a) for a in ("group", "x", "z", "c"))
    inputs = acts[0]
    upstream = cotangent[0]
    half = upstream.shape[1] // NC
    rows = inner_params.shape[1]

    *theirs_a, theirs_b = terms(inputs, upstream, 1 - core, x, z)
    got_a = []
    for a in theirs_a:
        got_a.append(swap(a, "c"))
    got_b = swap(theirs_b, "c")
    inputs, upstream, _ = lax.optimization_barrier((inputs, upstream, theirs_b))
    *own_a, own_b = terms(inputs, upstream, core, x, z)
    counts = group_tokens.astype(F32)
    steps = inner_steps.astype(F32)
    facts = jnp.stack(
        [
            counts / jnp.sum(counts),
            1.0 - jnp.power(F32(beta_one), steps),
            1.0 - jnp.power(F32(beta_two), steps),
        ],
        1,
    )
    facts = jnp.where(group == 0, facts, facts[::-1]).reshape(-1)

    near = (inner_params[0], adam_first[0], adam_second[0], anchor, momentum)

    def send(wire, n):
        return around(wire, "x", ORDER[n], NX)

    wire = (own_a[0] + got_a[0]).astype(WIRE)
    sent_0 = send(wire, 0)
    _, own_b, got_b = lax.optimization_barrier((wire, own_b, got_b))
    wire = [(own_b[k] + got_b[k]).astype(WIRE) for k in FAR]
    back_b = {}
    for k, w in zip(FAR, wire):
        back_b[k] = around(w, "z", k, NZ)
    second = own_b[0] + got_b[0]
    sent = [sent_0]
    for n in range(1, NX - 1):
        _, own, got = lax.optimization_barrier((wire, own_a[n], got_a[n]))
        wire = (own + got).astype(WIRE)
        sent.append(send(wire, n))
    gated, _ = lax.optimization_barrier((near, wire))
    packed = pl.pallas_call(
        pack_kernel,
        out_shape=jax.ShapeDtypeStruct(
            (sum(a.shape[0] for a in near), near[0].shape[1]), F32
        ),
        name="pack",
    )(*gated)
    far = swap(packed, "group")

    sent, far, facts = lax.optimization_barrier((sent, far, facts))
    first = own_a[-1] + got_a[-1]
    for w in sent:
        first = first + w.astype(F32)
    first = first * (1.0 / NX)
    wire = [first[k].astype(WIRE) for k in FAR]
    back_a = []
    for k, w in zip(FAR, wire):
        back_a.append(around(w, "z", k, NZ))
    first = first[0]
    for k in FAR:
        second = second + back_b[k].astype(F32)
    second = second * (1.0 / NZ)
    wires = [second[n].astype(WIRE) for n in range(NX - 1)]
    sent_b = [around(wires[n], "x", ORDER[n], NX) for n in range(NX - 1)]
    second = second[-1]
    sent_b, back_a = lax.optimization_barrier((sent_b, back_a))
    for w in sent_b:
        second = second + w.astype(F32)
    second = second * (1.0 / NX)
    for w in back_a:
        first = first + w.astype(F32)
    first = first * (1.0 / NZ)

    part = pl.pallas_call(
        turn_kernel,
        out_shape=jax.ShapeDtypeStruct((NG * NY * NC, rows, half), F32),
        name="turn",
    )(first, second)
    got = lax.all_to_all(part, ("group", "y", "c"), 0, 0, tiled=True)

    vmem = pl.BlockSpec(memory_space=pltpu.VMEM)
    smem = pl.BlockSpec(memory_space=pltpu.SMEM)
    new_anchor, new_momentum, weights = pl.pallas_call(
        final_kernel,
        in_specs=[smem, smem] + [vmem] * 7,
        out_specs=[vmem] * 3,
        out_shape=[
            jax.ShapeDtypeStruct(anchor.shape, F32),
            jax.ShapeDtypeStruct(anchor.shape, F32),
            jax.ShapeDtypeStruct((rows, anchor.shape[1]), jnp.bfloat16),
        ],
        name="final",
    )(group[None], facts, got, *near, far)
    return new_anchor, new_momentum, weights[None]


def solution(mesh):
    torus = Mesh(
        mesh.devices.reshape(NG, NX, NZ, NY, NC), ("group", "x", "z", "y", "c")
    )
    shard = P("group", FSDP, None)
    thin = P(FSDP_GROUP, None)

    return jax.shard_map(
        per_device,
        mesh=torus,
        in_specs=(shard, shard, shard, shard, shard, P(), P(), thin, thin),
        out_specs=(thin, thin, shard),
        check_vma=False,
    )
```

```python
import functools

import jax
import jax.numpy as jnp
from jax import lax
from jax.experimental import pallas as pl
from jax.experimental.pallas import tpu as pltpu
from jax.sharding import Mesh
from jax.sharding import PartitionSpec as P


FSDP = ("x", "z", "y", "c")
FSDP_GROUP = ("x", "z", "y", "c", "group")
NX, NZ, NY, NC, NG = 4, 8, 2, 2, 2

beta_one = 0.9
beta_two = 0.95
epsilon = 1e-08
inner_rate = 0.3
decay_rate = 0.1
outer_rate = 0.7
outer_mom = 0.9

WIRE = jnp.float16
F32 = jnp.float32
PEAK = 128.0
ROWS_A = 192
LANES = 128
BLOCK = 1024
AHEAD = 4
LIMIT = 28
ORDER = (2, 1, 3, 0)
FAR = (4, 3, 5, 2, 6, 1, 7)


def swap(a, axis):
    return lax.ppermute(a, axis, [(0, 1), (1, 0)])


def around(a, axis, k, size):
    return lax.ppermute(a, axis, [(i, (i + k) % size) for i in range(size)])


def terms_kernel(scale, core, place, layer, cot, acts, *refs):
    theirs, own = refs[: NX + 1], refs[NX + 1 : 2 * NX + 2]
    upstream, turned, held, kept, arrived, ready, left = refs[2 * NX + 2 :]
    steps = acts.shape[1] // BLOCK
    per = steps // NX
    half = upstream.shape[1] // NC
    turns = [n * per + i for n in (0, NX - 1, *range(1, NX - 1)) for i in range(per)]
    last = [
        pltpu.make_async_copy(kept.at[side], refs[NX - 1], left.at[side])
        if side == 0
        else pltpu.make_async_copy(kept.at[side], refs[2 * NX], left.at[side])
        for side in range(NC)
    ]

    def copy(i):
        x = lax.rem(place[0] + ORDER[i // per], NX)
        start = pl.multiple_of((x * per + i % per) * BLOCK, BLOCK)
        return pltpu.make_async_copy(
            acts.at[:, pl.ds(start, BLOCK)], held.at[i], arrived.at[i]
        )

    whole = pltpu.make_async_copy(cot, upstream, ready)
    whole.start()
    for i in turns[:AHEAD]:
        copy(i).start()
    whole.wait()
    for side in range(NC):
        which = lax.rem(core[0] + 1 + side, NC)
        part = upstream[:, pl.ds(pl.multiple_of(which * half, half), half)]
        turned[side * half : (side + 1) * half] = part.astype(F32).T.astype(part.dtype)
    for turn, i in enumerate(turns):
        copy(i).wait()
        if turn + AHEAD < steps:
            copy(turns[turn + AHEAD]).start()
        out = jnp.dot(turned[...], held[i], preferred_element_type=F32) * scale
        n = i // per
        for side, into in enumerate((theirs, own)):
            rows_a = kept.at[side] if n == NX - 1 else into[n]
            for j in range(BLOCK // LANES):
                z, y = divmod(j, NY)
                z += i % per * (NZ // per)
                piece = out[
                    side * half : (side + 1) * half, j * LANES : (j + 1) * LANES
                ]
                rows_a[lax.rem(z + NZ - layer[0], NZ), y] = piece[:ROWS_A]
                into[NX][z, n, y] = piece[ROWS_A:]
        if turn == 2 * per - 1:
            for c in last:
                c.start()
    for c in last:
        c.wait()


def terms(inputs, upstream, core, x, z):
    tokens, width = inputs.shape
    keys = upstream.shape[1]
    half = keys // NC
    steps = width // BLOCK
    vmem = pl.BlockSpec(memory_space=pltpu.VMEM)
    block_a = (NZ, NY, ROWS_A, LANES)
    out = pl.pallas_call(
        functools.partial(terms_kernel, PEAK / (tokens * NC)),
        in_specs=[pl.BlockSpec(memory_space=pltpu.SMEM)] * 3
        + [pl.BlockSpec(memory_space=pl.ANY)] * 2,
        out_specs=([vmem] * (NX - 1) + [pl.BlockSpec(memory_space=pl.ANY), vmem]) * NC,
        scratch_shapes=[
            pltpu.VMEM((tokens, keys), inputs.dtype),
            pltpu.VMEM((keys, tokens), inputs.dtype),
            pltpu.VMEM((steps, tokens, BLOCK), inputs.dtype),
            pltpu.VMEM((NC,) + block_a, F32),
            pltpu.SemaphoreType.DMA((steps,)),
            pltpu.SemaphoreType.DMA,
            pltpu.SemaphoreType.DMA((NC,)),
        ],
        out_shape=(
            [pltpu.VMEM(block_a, F32)] * (NX - 1)
            + [pltpu.HBM(block_a, F32)]
            + [pltpu.VMEM((NZ, NX, NY, half - ROWS_A, LANES), F32)]
        )
        * NC,
        compiler_params=pltpu.CompilerParams(vmem_limit_bytes=LIMIT * 2**20),
        cost_estimate=pl.CostEstimate(
            flops=2 * tokens * keys * width,
            bytes_accessed=2 * tokens * width + 4 * keys * width,
            transcendentals=0,
        ),
        name="terms",
    )(
        core[None],
        x[None],
        z[None],
        pltpu.with_memory_space_constraint(upstream, pltpu.HBM),
        pltpu.with_memory_space_constraint(inputs, pltpu.HBM),
    )
    return out[:NX], out[NX], out[NX + 1 : 2 * NX + 1], out[2 * NX + 1]


def turn_kernel(first, second, out):
    rows = LANES // NC
    for y in range(NY):
        whole = jnp.concatenate([first[y], second[y]], 0).T
        for c in range(NC):
            for g in range(NG):
                out[(g * NY + y) * NC + c] = whole[c * rows : (c + 1) * rows]


def pack_kernel(*refs):
    at = 0
    for ref in refs[:-1]:
        refs[-1][at : at + ref.shape[0]] = ref[...]
        at += ref.shape[0]


def final_kernel(group, facts, got, p0, m0, v0, a0, w0, far, new_a, new_m, new_w):
    rows, few = p0.shape[0], a0.shape[0]
    p1, m1, v1 = (far[i * rows : (i + 1) * rows] for i in range(3))
    a1, w1 = far[3 * rows : 3 * rows + few], far[3 * rows + few :]
    mine = group[0] == 0

    def weighted(first, k, p, m, v):
        at = [(g * NY + y) * NC for g in range(NG) for y in range(NY)]
        sides = []
        for c in range(NC):
            zero = got[at[0] + c] + got[at[1] + c]
            one = got[at[2] + c] + got[at[3] + c]
            sides.append(jnp.where(mine == first, zero, one))
        gradient = jnp.concatenate(sides, -1) * (1.0 / (NY * PEAK))
        share, correct_one, correct_two = (facts[3 * k + n] for n in range(3))
        fresh_first = beta_one * m + (1.0 - beta_one) * gradient
        fresh_second = beta_two * v + (1.0 - beta_two) * gradient * gradient
        ratio = (
            fresh_first / correct_one / (jnp.sqrt(fresh_second / correct_two) + epsilon)
        )
        return share * (p - inner_rate * (ratio + decay_rate * p))

    merged = weighted(True, 0, p0[...], m0[...], v0[...]) + weighted(
        False, 1, p1, m1, v1
    )

    def half(anchor, momentum, part):
        pseudo = anchor - part
        fresh_momentum = outer_mom * momentum + pseudo
        fresh_anchor = anchor - outer_rate * (pseudo + outer_mom * fresh_momentum)
        return fresh_anchor, fresh_momentum

    front, back = merged[:few], merged[few:]
    near_anchor, near_momentum = half(a0[...], w0[...], jnp.where(mine, front, back))
    far_anchor, _ = half(a1, w1, jnp.where(mine, back, front))
    new_a[...] = near_anchor
    new_m[...] = near_momentum
    new_w[:few] = jnp.where(mine, near_anchor, far_anchor).astype(new_w.dtype)
    new_w[few:] = jnp.where(mine, far_anchor, near_anchor).astype(new_w.dtype)


def per_device(
    acts,
    cotangent,
    inner_params,
    adam_first,
    adam_second,
    inner_steps,
    group_tokens,
    anchor,
    momentum,
):
    group, x, z, core = (lax.axis_index(a) for a in ("group", "x", "z", "c"))
    inputs = acts[0]
    upstream = cotangent[0]
    half = upstream.shape[1] // NC
    rows = inner_params.shape[1]

    theirs_a, theirs_b, own_a, own_b = terms(inputs, upstream, core, x, z)
    got_a = []
    for a in theirs_a:
        got_a.append(swap(a, "c"))
    got_b = swap(theirs_b, "c")
    counts = group_tokens.astype(F32)
    steps = inner_steps.astype(F32)
    facts = jnp.stack(
        [
            counts / jnp.sum(counts),
            1.0 - jnp.power(F32(beta_one), steps),
            1.0 - jnp.power(F32(beta_two), steps),
        ],
        1,
    )
    facts = jnp.where(group == 0, facts, facts[::-1]).reshape(-1)

    near = (inner_params[0], adam_first[0], adam_second[0], anchor, momentum)

    def send(wire, n):
        return around(wire, "x", ORDER[n], NX)

    wire = (own_a[0] + got_a[0]).astype(WIRE)
    sent_0 = send(wire, 0)
    _, own_b, got_b = lax.optimization_barrier((wire, own_b, got_b))
    wire = (own_b + got_b).astype(WIRE)
    back_b = lax.all_to_all(wire, "z", 0, 0, tiled=True)
    sent = [sent_0]
    for n in range(1, NX - 1):
        _, own, got = lax.optimization_barrier((wire, own_a[n], got_a[n]))
        wire = (own + got).astype(WIRE)
        sent.append(send(wire, n))
    gated, _ = lax.optimization_barrier((near, wire))
    packed = pl.pallas_call(
        pack_kernel,
        out_shape=jax.ShapeDtypeStruct(
            (sum(a.shape[0] for a in near), near[0].shape[1]), F32
        ),
        name="pack",
    )(*gated)
    far = swap(packed, "group")

    sent, back_b, far, facts = lax.optimization_barrier(
        (sent, back_b, far, facts)
    )
    first = own_a[-1] + got_a[-1]
    for w in sent:
        first = first + w.astype(F32)
    first = first * (1.0 / NX)
    wire = [first[k].astype(WIRE) for k in FAR]
    back_a = []
    for k, w in zip(FAR, wire):
        back_a.append(around(w, "z", k, NZ))
    first = first[0]
    second = back_b.astype(F32).sum(0) * (1.0 / NZ)
    wires = [second[n].astype(WIRE) for n in range(NX - 1)]
    sent_b = [around(wires[n], "x", ORDER[n], NX) for n in range(NX - 1)]
    second = second[-1]
    sent_b, back_a = lax.optimization_barrier((sent_b, back_a))
    for w in sent_b:
        second = second + w.astype(F32)
    second = second * (1.0 / NX)
    for w in back_a:
        first = first + w.astype(F32)
    first = first * (1.0 / NZ)

    part = pl.pallas_call(
        turn_kernel,
        out_shape=jax.ShapeDtypeStruct((NG * NY * NC, rows, half), F32),
        name="turn",
    )(first, second)
    got = lax.all_to_all(part, ("group", "y", "c"), 0, 0, tiled=True)

    vmem = pl.BlockSpec(memory_space=pltpu.VMEM)
    smem = pl.BlockSpec(memory_space=pltpu.SMEM)
    new_anchor, new_momentum, weights = pl.pallas_call(
        final_kernel,
        in_specs=[smem, smem] + [vmem] * 7,
        out_specs=[vmem] * 3,
        out_shape=[
            jax.ShapeDtypeStruct(anchor.shape, F32),
            jax.ShapeDtypeStruct(anchor.shape, F32),
            jax.ShapeDtypeStruct((rows, anchor.shape[1]), jnp.bfloat16),
        ],
        name="final",
    )(group[None], facts, got, *near, far)
    return new_anchor, new_momentum, weights[None]


def solution(mesh):
    torus = Mesh(
        mesh.devices.reshape(NG, NX, NZ, NY, NC), ("group", "x", "z", "y", "c")
    )
    shard = P("group", FSDP, None)
    thin = P(FSDP_GROUP, None)

    return jax.shard_map(
        per_device,
        mesh=torus,
        in_specs=(shard, shard, shard, shard, shard, P(), P(), thin, thin),
        out_specs=(thin, thin, shard),
        check_vma=False,
    )
```

```python
import functools

import jax
import jax.numpy as jnp
from jax import lax
from jax.experimental import pallas as pl
from jax.experimental.pallas import tpu as pltpu
from jax.sharding import Mesh
from jax.sharding import PartitionSpec as P


FSDP = ("x", "z", "y", "c")
FSDP_GROUP = ("x", "z", "y", "c", "group")
NX, NZ, NY, NC, NG = 4, 8, 2, 2, 2

beta_one = 0.9
beta_two = 0.95
epsilon = 1e-08
inner_rate = 0.3
decay_rate = 0.1
outer_rate = 0.7
outer_mom = 0.9

WIRE = jnp.float16
F32 = jnp.float32
PEAK = 128.0
ROWS_A = 192
LANES = 128
BLOCK = 1024
AHEAD = 4
LIMIT = 28
ORDER = (2, 1, 3, 0)
FAR = (4, 3, 5, 2, 6, 1, 7)


def on_chip(*arrays):
    return [pltpu.with_memory_space_constraint(a, pltpu.VMEM) for a in arrays]


def swap(a, axis):
    return lax.ppermute(a, axis, [(0, 1), (1, 0)])


def around(a, axis, k, size):
    return lax.ppermute(a, axis, [(i, (i + k) % size) for i in range(size)])


def terms_kernel(scale, core, place, layer, cot, acts, *refs):
    theirs, own = refs[: NX + 1], refs[NX + 1 : 2 * NX + 2]
    upstream, turned, held, kept, arrived, ready, left = refs[2 * NX + 2 :]
    steps = acts.shape[1] // BLOCK
    per = steps // NX
    half = upstream.shape[1] // NC
    turns = [n * per + i for n in (0, NX - 1, *range(1, NX - 1)) for i in range(per)]
    last = [
        pltpu.make_async_copy(kept.at[side], refs[NX - 1], left.at[side])
        if side == 0
        else pltpu.make_async_copy(kept.at[side], refs[2 * NX], left.at[side])
        for side in range(NC)
    ]

    def copy(i):
        x = lax.rem(place[0] + ORDER[i // per], NX)
        start = pl.multiple_of((x * per + i % per) * BLOCK, BLOCK)
        return pltpu.make_async_copy(
            acts.at[:, pl.ds(start, BLOCK)], held.at[i], arrived.at[i]
        )

    whole = pltpu.make_async_copy(cot, upstream, ready)
    whole.start()
    for i in turns[:AHEAD]:
        copy(i).start()
    whole.wait()
    for side in range(NC):
        which = lax.rem(core[0] + 1 + side, NC)
        part = upstream[:, pl.ds(pl.multiple_of(which * half, half), half)]
        turned[side * half : (side + 1) * half] = part.astype(F32).T.astype(part.dtype)
    for turn, i in enumerate(turns):
        copy(i).wait()
        if turn + AHEAD < steps:
            copy(turns[turn + AHEAD]).start()
        out = jnp.dot(turned[...], held[i], preferred_element_type=F32) * scale
        n = i // per
        for side, into in enumerate((theirs, own)):
            rows_a = kept.at[side] if n == NX - 1 else into[n]
            for j in range(BLOCK // LANES):
                z, y = divmod(j, NY)
                z += i % per * (NZ // per)
                piece = out[
                    side * half : (side + 1) * half, j * LANES : (j + 1) * LANES
                ]
                rows_a[lax.rem(z + NZ - layer[0], NZ), y] = piece[:ROWS_A]
                into[NX][z, n, y] = piece[ROWS_A:]
        if turn == 2 * per - 1:
            for c in last:
                c.start()
    for c in last:
        c.wait()


def terms(inputs, upstream, core, x, z):
    tokens, width = inputs.shape
    keys = upstream.shape[1]
    half = keys // NC
    steps = width // BLOCK
    vmem = pl.BlockSpec(memory_space=pltpu.VMEM)
    block_a = (NZ, NY, ROWS_A, LANES)
    out = pl.pallas_call(
        functools.partial(terms_kernel, PEAK / (tokens * NC)),
        in_specs=[pl.BlockSpec(memory_space=pltpu.SMEM)] * 3
        + [pl.BlockSpec(memory_space=pl.ANY)] * 2,
        out_specs=([vmem] * (NX - 1) + [pl.BlockSpec(memory_space=pl.ANY), vmem]) * NC,
        scratch_shapes=[
            pltpu.VMEM((tokens, keys), inputs.dtype),
            pltpu.VMEM((keys, tokens), inputs.dtype),
            pltpu.VMEM((steps, tokens, BLOCK), inputs.dtype),
            pltpu.VMEM((NC,) + block_a, F32),
            pltpu.SemaphoreType.DMA((steps,)),
            pltpu.SemaphoreType.DMA,
            pltpu.SemaphoreType.DMA((NC,)),
        ],
        out_shape=(
            [pltpu.VMEM(block_a, F32)] * (NX - 1)
            + [pltpu.HBM(block_a, F32)]
            + [pltpu.VMEM((NZ, NX, NY, half - ROWS_A, LANES), F32)]
        )
        * NC,
        compiler_params=pltpu.CompilerParams(vmem_limit_bytes=LIMIT * 2**20),
        cost_estimate=pl.CostEstimate(
            flops=2 * tokens * keys * width,
            bytes_accessed=2 * tokens * width + 4 * keys * width,
            transcendentals=0,
        ),
        name="terms",
    )(
        core[None],
        x[None],
        z[None],
        pltpu.with_memory_space_constraint(upstream, pltpu.HBM),
        pltpu.with_memory_space_constraint(inputs, pltpu.HBM),
    )
    return out[:NX], out[NX], out[NX + 1 : 2 * NX + 1], out[2 * NX + 1]


def turn_kernel(first, second, out):
    rows = LANES // NC
    for y in range(NY):
        whole = jnp.concatenate([first[y], second[y]], 0).T
        for c in range(NC):
            for g in range(NG):
                out[(g * NY + y) * NC + c] = whole[c * rows : (c + 1) * rows]


def pack_kernel(*refs):
    at = 0
    for ref in refs[:-1]:
        refs[-1][at : at + ref.shape[0]] = ref[...]
        at += ref.shape[0]


def final_kernel(group, facts, got, p0, m0, v0, a0, w0, far, new_a, new_m, new_w):
    rows, few = p0.shape[0], a0.shape[0]
    p1, m1, v1 = (far[i * rows : (i + 1) * rows] for i in range(3))
    a1, w1 = far[3 * rows : 3 * rows + few], far[3 * rows + few :]
    mine = group[0] == 0

    def weighted(first, k, p, m, v):
        at = [(g * NY + y) * NC for g in range(NG) for y in range(NY)]
        sides = []
        for c in range(NC):
            zero = got[at[0] + c] + got[at[1] + c]
            one = got[at[2] + c] + got[at[3] + c]
            sides.append(jnp.where(mine == first, zero, one))
        gradient = jnp.concatenate(sides, -1) * (1.0 / (NY * PEAK))
        share, correct_one, correct_two = (facts[3 * k + n] for n in range(3))
        fresh_first = beta_one * m + (1.0 - beta_one) * gradient
        fresh_second = beta_two * v + (1.0 - beta_two) * gradient * gradient
        ratio = (
            fresh_first / correct_one / (jnp.sqrt(fresh_second / correct_two) + epsilon)
        )
        return share * (p - inner_rate * (ratio + decay_rate * p))

    merged = weighted(True, 0, p0[...], m0[...], v0[...]) + weighted(
        False, 1, p1, m1, v1
    )

    def half(anchor, momentum, part):
        pseudo = anchor - part
        fresh_momentum = outer_mom * momentum + pseudo
        fresh_anchor = anchor - outer_rate * (pseudo + outer_mom * fresh_momentum)
        return fresh_anchor, fresh_momentum

    front, back = merged[:few], merged[few:]
    near_anchor, near_momentum = half(a0[...], w0[...], jnp.where(mine, front, back))
    far_anchor, _ = half(a1, w1, jnp.where(mine, back, front))
    new_a[...] = near_anchor
    new_m[...] = near_momentum
    new_w[:few] = jnp.where(mine, near_anchor, far_anchor).astype(new_w.dtype)
    new_w[few:] = jnp.where(mine, far_anchor, near_anchor).astype(new_w.dtype)


def per_device(
    acts,
    cotangent,
    inner_params,
    adam_first,
    adam_second,
    inner_steps,
    group_tokens,
    anchor,
    momentum,
):
    group, x, z, core = (lax.axis_index(a) for a in ("group", "x", "z", "c"))
    inputs = acts[0]
    upstream = cotangent[0]
    half = upstream.shape[1] // NC
    rows = inner_params.shape[1]

    theirs_a, theirs_b, own_a, own_b = terms(inputs, upstream, core, x, z)
    got_a = []
    for a in theirs_a:
        got_a.append(swap(a, "c"))
    got_b = swap(theirs_b, "c")
    counts = group_tokens.astype(F32)
    steps = inner_steps.astype(F32)
    facts = jnp.stack(
        [
            counts / jnp.sum(counts),
            1.0 - jnp.power(F32(beta_one), steps),
            1.0 - jnp.power(F32(beta_two), steps),
        ],
        1,
    )
    facts = jnp.where(group == 0, facts, facts[::-1]).reshape(-1)

    near = (inner_params[0], adam_first[0], adam_second[0], anchor, momentum)

    def send(wire, n):
        return around(wire, "x", ORDER[n], NX)

    wire = (own_a[0] + got_a[0]).astype(WIRE)
    sent_0 = send(wire, 0)
    _, own_b, got_b = lax.optimization_barrier((wire, own_b, got_b))
    wire = (own_b + got_b).astype(WIRE)
    back_b = lax.all_to_all(wire, "z", 0, 0, tiled=True)
    sent = [sent_0]
    for n in range(1, NX - 1):
        _, own, got = lax.optimization_barrier((wire, own_a[n], got_a[n]))
        wire = (own + got).astype(WIRE)
        sent.append(send(wire, n))
    gated, _ = lax.optimization_barrier((near, wire))
    packed = pl.pallas_call(
        pack_kernel,
        out_shape=jax.ShapeDtypeStruct(
            (sum(a.shape[0] for a in near), near[0].shape[1]), F32
        ),
        name="pack",
    )(*gated)
    far = swap(packed, "group")

    sent, back_b, far, facts = lax.optimization_barrier(
        (sent, back_b, far, facts)
    )
    first = own_a[-1] + got_a[-1]
    for w in sent:
        first = first + w.astype(F32)
    first = first * (1.0 / NX)
    wire = [first[k].astype(WIRE) for k in FAR]
    back_a = []
    for k, w in zip(FAR, wire):
        back_a.append(around(w, "z", k, NZ))
    first = first[0]
    second = back_b.astype(F32).sum(0) * (1.0 / NZ)
    wires = [second[n].astype(WIRE) for n in range(NX - 1)]
    sent_b = [around(wires[n], "x", ORDER[n], NX) for n in range(NX - 1)]
    second = second[-1]
    sent_b, back_a = lax.optimization_barrier((sent_b, back_a))
    for w in sent_b:
        second = second + w.astype(F32)
    second = second * (1.0 / NX)
    for w in back_a:
        first = first + w.astype(F32)
    first = first * (1.0 / NZ)

    part = pl.pallas_call(
        turn_kernel,
        in_specs=[pl.BlockSpec(memory_space=pltpu.VMEM)] * 2,
        out_specs=pl.BlockSpec(memory_space=pltpu.VMEM),
        out_shape=pltpu.VMEM((NG * NY * NC, rows, half), F32),
        name="turn",
    )(*on_chip(first, second))
    got = lax.all_to_all(part, ("group", "y", "c"), 0, 0, tiled=True)

    vmem = pl.BlockSpec(memory_space=pltpu.VMEM)
    smem = pl.BlockSpec(memory_space=pltpu.SMEM)
    new_anchor, new_momentum, weights = pl.pallas_call(
        final_kernel,
        in_specs=[smem, smem] + [vmem] * 7,
        out_specs=[vmem] * 3,
        out_shape=[
            jax.ShapeDtypeStruct(anchor.shape, F32),
            jax.ShapeDtypeStruct(anchor.shape, F32),
            jax.ShapeDtypeStruct((rows, anchor.shape[1]), jnp.bfloat16),
        ],
        name="final",
    )(group[None], facts, *on_chip(got, *near, far))
    return new_anchor, new_momentum, weights[None]


def solution(mesh):
    torus = Mesh(
        mesh.devices.reshape(NG, NX, NZ, NY, NC), ("group", "x", "z", "y", "c")
    )
    shard = P("group", FSDP, None)
    thin = P(FSDP_GROUP, None)

    return jax.shard_map(
        per_device,
        mesh=torus,
        in_specs=(shard, shard, shard, shard, shard, P(), P(), thin, thin),
        out_specs=(thin, thin, shard),
        check_vma=False,
    )
```

```python
import functools

import jax
import jax.numpy as jnp
from jax import lax
from jax.experimental import pallas as pl
from jax.experimental.pallas import tpu as pltpu
from jax.sharding import Mesh
from jax.sharding import PartitionSpec as P


FSDP = ("x", "z", "y", "c")
FSDP_GROUP = ("x", "z", "y", "c", "group")
NX, NZ, NY, NC, NG = 4, 8, 2, 2, 2

beta_one = 0.9
beta_two = 0.95
epsilon = 1e-08
inner_rate = 0.3
decay_rate = 0.1
outer_rate = 0.7
outer_mom = 0.9

WIRE = jnp.float16
F32 = jnp.float32
PEAK = 128.0
ROWS_A = 192
LANES = 128
BLOCK = 1024
LIMIT = 28
ORDER = (2, 1, 3, 0)
FAR = (4, 3, 5, 2, 6, 1, 7)


def on_chip(*arrays):
    return [pltpu.with_memory_space_constraint(a, pltpu.VMEM) for a in arrays]


def swap(a, axis):
    return lax.ppermute(a, axis, [(0, 1), (1, 0)])


def around(a, axis, k, size):
    return lax.ppermute(a, axis, [(i, (i + k) % size) for i in range(size)])


def terms_kernel(scale, core, place, layer, cot, acts, *refs):
    theirs, own = refs[: NX + 1], refs[NX + 1 : 2 * NX + 2]
    upstream, turned, held, kept, arrived, ready, left = refs[2 * NX + 2 :]
    steps = acts.shape[1] // BLOCK
    per = steps // NX
    half = upstream.shape[1] // NC
    turns = (0, NX - 1, *range(1, NX - 1))
    last = [
        pltpu.make_async_copy(kept.at[side], refs[NX - 1], left.at[side])
        if side == 0
        else pltpu.make_async_copy(kept.at[side], refs[2 * NX], left.at[side])
        for side in range(NC)
    ]

    def copy(n, b):
        x = lax.rem(place[0] + ORDER[n], NX)
        start = pl.multiple_of((x * per + b) * BLOCK, BLOCK)
        return pltpu.make_async_copy(
            acts.at[:, pl.ds(start, BLOCK)],
            held.at[n * per + b],
            arrived.at[n * per + b],
        )

    whole = pltpu.make_async_copy(cot, upstream, ready)
    whole.start()
    for b in range(per):
        copy(turns[0], b).start()
    whole.wait()
    for side in range(NC):
        which = lax.rem(core[0] + 1 + side, NC)
        part = upstream[:, pl.ds(pl.multiple_of(which * half, half), half)]
        turned[side * half : (side + 1) * half] = part.astype(F32).T.astype(part.dtype)
    for n in turns[1:]:
        for b in range(per):
            copy(n, b).start()
    for n in turns:

        @pl.loop(0, per)
        def _(b):
            copy(n, b).wait()
            block = held[n * per + b]
            out = jnp.dot(turned[...], block, preferred_element_type=F32) * scale
            for side, into in enumerate((theirs, own)):
                rows_a = kept.at[side] if n == NX - 1 else into[n]
                for j in range(BLOCK // LANES):
                    z, y = divmod(j, NY)
                    z += b * (NZ // per)
                    piece = out[
                        side * half : (side + 1) * half, j * LANES : (j + 1) * LANES
                    ]
                    rows_a[lax.rem(z + NZ - layer[0], NZ), y] = piece[:ROWS_A]
                    into[NX][z, n, y] = piece[ROWS_A:]

        if n == NX - 1:
            for c in last:
                c.start()
    for c in last:
        c.wait()


def terms(inputs, upstream, core, x, z):
    tokens, width = inputs.shape
    keys = upstream.shape[1]
    half = keys // NC
    steps = width // BLOCK
    vmem = pl.BlockSpec(memory_space=pltpu.VMEM)
    block_a = (NZ, NY, ROWS_A, LANES)
    out = pl.pallas_call(
        functools.partial(terms_kernel, PEAK / (tokens * NC)),
        in_specs=[pl.BlockSpec(memory_space=pltpu.SMEM)] * 3
        + [pl.BlockSpec(memory_space=pl.ANY)] * 2,
        out_specs=([vmem] * (NX - 1) + [pl.BlockSpec(memory_space=pl.ANY), vmem]) * NC,
        scratch_shapes=[
            pltpu.VMEM((tokens, keys), inputs.dtype),
            pltpu.VMEM((keys, tokens), inputs.dtype),
            pltpu.VMEM((steps, tokens, BLOCK), inputs.dtype),
            pltpu.VMEM((NC,) + block_a, F32),
            pltpu.SemaphoreType.DMA((steps,)),
            pltpu.SemaphoreType.DMA,
            pltpu.SemaphoreType.DMA((NC,)),
        ],
        out_shape=(
            [pltpu.VMEM(block_a, F32)] * (NX - 1)
            + [pltpu.HBM(block_a, F32)]
            + [pltpu.VMEM((NZ, NX, NY, half - ROWS_A, LANES), F32)]
        )
        * NC,
        compiler_params=pltpu.CompilerParams(vmem_limit_bytes=LIMIT * 2**20),
        cost_estimate=pl.CostEstimate(
            flops=2 * tokens * keys * width,
            bytes_accessed=2 * tokens * width + 4 * keys * width,
            transcendentals=0,
        ),
        name="terms",
    )(
        core[None],
        x[None],
        z[None],
        pltpu.with_memory_space_constraint(upstream, pltpu.HBM),
        pltpu.with_memory_space_constraint(inputs, pltpu.HBM),
    )
    return out[:NX], out[NX], out[NX + 1 : 2 * NX + 1], out[2 * NX + 1]


def turn_kernel(first, second, out):
    rows = LANES // NC
    for y in range(NY):
        whole = jnp.concatenate([first[y], second[y]], 0).T
        for c in range(NC):
            for g in range(NG):
                out[(g * NY + y) * NC + c] = whole[c * rows : (c + 1) * rows]


def pack_kernel(*refs):
    at = 0
    for ref in refs[:-1]:
        refs[-1][at : at + ref.shape[0]] = ref[...]
        at += ref.shape[0]


def final_kernel(group, facts, got, p0, m0, v0, a0, w0, far, new_a, new_m, new_w):
    rows, few = p0.shape[0], a0.shape[0]
    p1, m1, v1 = (far[i * rows : (i + 1) * rows] for i in range(3))
    a1, w1 = far[3 * rows : 3 * rows + few], far[3 * rows + few :]
    mine = group[0] == 0

    def weighted(first, k, p, m, v):
        at = [(g * NY + y) * NC for g in range(NG) for y in range(NY)]
        sides = []
        for c in range(NC):
            zero = got[at[0] + c] + got[at[1] + c]
            one = got[at[2] + c] + got[at[3] + c]
            sides.append(jnp.where(mine == first, zero, one))
        gradient = jnp.concatenate(sides, -1) * (1.0 / (NY * PEAK))
        share, correct_one, correct_two = (facts[3 * k + n] for n in range(3))
        fresh_first = beta_one * m + (1.0 - beta_one) * gradient
        fresh_second = beta_two * v + (1.0 - beta_two) * gradient * gradient
        ratio = (
            fresh_first / correct_one / (jnp.sqrt(fresh_second / correct_two) + epsilon)
        )
        return share * (p - inner_rate * (ratio + decay_rate * p))

    merged = weighted(True, 0, p0[...], m0[...], v0[...]) + weighted(
        False, 1, p1, m1, v1
    )

    def half(anchor, momentum, part):
        pseudo = anchor - part
        fresh_momentum = outer_mom * momentum + pseudo
        fresh_anchor = anchor - outer_rate * (pseudo + outer_mom * fresh_momentum)
        return fresh_anchor, fresh_momentum

    front, back = merged[:few], merged[few:]
    near_anchor, near_momentum = half(a0[...], w0[...], jnp.where(mine, front, back))
    far_anchor, _ = half(a1, w1, jnp.where(mine, back, front))
    new_a[...] = near_anchor
    new_m[...] = near_momentum
    new_w[:few] = jnp.where(mine, near_anchor, far_anchor).astype(new_w.dtype)
    new_w[few:] = jnp.where(mine, far_anchor, near_anchor).astype(new_w.dtype)


def per_device(
    acts,
    cotangent,
    inner_params,
    adam_first,
    adam_second,
    inner_steps,
    group_tokens,
    anchor,
    momentum,
):
    group, x, z, core = (lax.axis_index(a) for a in ("group", "x", "z", "c"))
    inputs = acts[0]
    upstream = cotangent[0]
    half = upstream.shape[1] // NC
    rows = inner_params.shape[1]

    theirs_a, theirs_b, own_a, own_b = terms(inputs, upstream, core, x, z)
    got_a = []
    for a in theirs_a:
        got_a.append(swap(a, "c"))
    got_b = swap(theirs_b, "c")
    counts = group_tokens.astype(F32)
    steps = inner_steps.astype(F32)
    facts = jnp.stack(
        [
            counts / jnp.sum(counts),
            1.0 - jnp.power(F32(beta_one), steps),
            1.0 - jnp.power(F32(beta_two), steps),
        ],
        1,
    )
    facts = jnp.where(group == 0, facts, facts[::-1]).reshape(-1)

    near = (inner_params[0], adam_first[0], adam_second[0], anchor, momentum)

    def send(wire, n):
        return around(wire, "x", ORDER[n], NX)

    wire = (own_a[0] + got_a[0]).astype(WIRE)
    sent_0 = send(wire, 0)
    _, own_b, got_b = lax.optimization_barrier((wire, own_b, got_b))
    wire = (own_b + got_b).astype(WIRE)
    back_b = lax.all_to_all(wire, "z", 0, 0, tiled=True)
    sent = [sent_0]
    for n in range(1, NX - 1):
        _, own, got = lax.optimization_barrier((wire, own_a[n], got_a[n]))
        wire = (own + got).astype(WIRE)
        sent.append(send(wire, n))
    gated, _ = lax.optimization_barrier((near, wire))
    packed = pl.pallas_call(
        pack_kernel,
        out_shape=jax.ShapeDtypeStruct(
            (sum(a.shape[0] for a in near), near[0].shape[1]), F32
        ),
        name="pack",
    )(*gated)
    far = swap(packed, "group")

    sent, back_b, far, facts = lax.optimization_barrier(
        (sent, back_b, far, facts)
    )
    first = own_a[-1] + got_a[-1]
    for w in sent:
        first = first + w.astype(F32)
    first = first * (1.0 / NX)
    wire = [first[k].astype(WIRE) for k in FAR]
    back_a = []
    for k, w in zip(FAR, wire):
        back_a.append(around(w, "z", k, NZ))
    first = first[0]
    second = back_b.astype(F32).sum(0) * (1.0 / NZ)
    wires = [second[n].astype(WIRE) for n in range(NX - 1)]
    sent_b = [around(wires[n], "x", ORDER[n], NX) for n in range(NX - 1)]
    second = second[-1]
    sent_b, back_a = lax.optimization_barrier((sent_b, back_a))
    for w in sent_b:
        second = second + w.astype(F32)
    second = second * (1.0 / NX)
    for w in back_a:
        first = first + w.astype(F32)
    first = first * (1.0 / NZ)

    part = pl.pallas_call(
        turn_kernel,
        in_specs=[pl.BlockSpec(memory_space=pltpu.VMEM)] * 2,
        out_specs=pl.BlockSpec(memory_space=pltpu.VMEM),
        out_shape=pltpu.VMEM((NG * NY * NC, rows, half), F32),
        name="turn",
    )(*on_chip(first, second))
    got = lax.all_to_all(part, ("group", "y", "c"), 0, 0, tiled=True)

    vmem = pl.BlockSpec(memory_space=pltpu.VMEM)
    smem = pl.BlockSpec(memory_space=pltpu.SMEM)
    new_anchor, new_momentum, weights = pl.pallas_call(
        final_kernel,
        in_specs=[smem, smem] + [vmem] * 7,
        out_specs=[vmem] * 3,
        out_shape=[
            jax.ShapeDtypeStruct(anchor.shape, F32),
            jax.ShapeDtypeStruct(anchor.shape, F32),
            jax.ShapeDtypeStruct((rows, anchor.shape[1]), jnp.bfloat16),
        ],
        name="final",
    )(group[None], facts, *on_chip(got, *near, far))
    return new_anchor, new_momentum, weights[None]


def solution(mesh):
    torus = Mesh(
        mesh.devices.reshape(NG, NX, NZ, NY, NC), ("group", "x", "z", "y", "c")
    )
    shard = P("group", FSDP, None)
    thin = P(FSDP_GROUP, None)

    return jax.shard_map(
        per_device,
        mesh=torus,
        in_specs=(shard, shard, shard, shard, shard, P(), P(), thin, thin),
        out_specs=(thin, thin, shard),
        check_vma=False,
    )
```
